32 devices in a mesh: dp: 4 (over z), group: 8 (over y, x, core).
Axes of the slice: x: 2, y: 2, z: 4, core: 2. Of those that a mesh axis runs over, the one named last changes fastest.
Arguments:
- points: bfloat16 [262144, 1024], P(('dp', 'group')), may hold values from -12 to 12
- block_rows: int32 [2048], P(('dp', 'group')), may hold values from 1 to 128
- block_owner: int32 [2048, 1], P(('dp', 'group')), may hold values from 0 to 31; in each aligned block of 64 rows (0 to 63, 64 to 127, ...) at most 2 rows name the same one
- block_local: int32 [2048], P(('dp', 'group')), may hold values from 0 to 7
- assign_mid: int32 [256, 1], P(('dp', 'group')), may hold values from 0 to 255
- assign_top: int32 [256, 1], P('group'), may hold values from 0 to 255
Outputs:
- level1: float32 [256, 1024], P(('dp', 'group'))
- best: float32 [262144], P(('dp', 'group'))
- level2: float32 [256, 1024], P('group')
- level3: float32 [256, 1024], replicated
The draws below stay inside these ranges and needn't reach their ends.
Inputs may be any that keep to these rules, and one draw needn't show every extreme that they name: `block_owner`: among the blocks of one device, no owner is named more than 2 times. `assign_mid`: every level-2 cluster is named by at least one level-1 centroid. `assign_top`: every level-3 cluster is named by at least one level-2 centroid.
All inputs are finite; a program needn't handle non-finite values.
Results may differ from the reference program's by a relative error of at most 0.0014.
Values may be sent and summed in bfloat16 or wider, within the bound.
No kernel may reach another device: no remote copies, remote signals or barrier semaphores. Data moves between devices by JAX's collectives and lax.ppermute only.
A program may use at most 64 MiB of HBM per device.

```python
import math
import jax
import jax.numpy as jnp
import numpy as np
from jax import lax

D = 1024
BLOCK = 128
SLOTS = 2
P_DEV = 8192
K1_DEV = 8
K3 = 256
K1 = 256
K2 = 256
POINTS = 262144
BLOCKS = 2048
DEVICES = 32


def place_ends(result, stream_key, least, top_value):
    index_at = [jax.random.randint(jax.random.fold_in(stream_key, axis), (), 0, length) for axis, length in enumerate(result.shape)]
    widest = result.shape.index(max(result.shape))
    neighbour = index_at[:widest] + [(index_at[widest] + 1) % result.shape[widest]] + index_at[widest + 1:]
    return result.at[tuple(index_at)].set(least).at[tuple(neighbour)].set(top_value)


def block_levels(stream_key, shape, pieces, low, top_value):
    level, own = 1.0, jax.random.fold_in(stream_key, 6)
    for dim, parts in pieces:
        draws = jnp.exp(jax.random.uniform(jax.random.fold_in(own, dim), (parts,), jnp.float32, low / len(pieces), top_value / len(pieces)))
        level = level * jnp.repeat(draws, shape[dim] // parts).reshape([-1 if axis == dim else 1 for axis in range(len(shape))])
    return level


def picks_of(own_key, rows, count, top, lift):
    sequence = jax.random.permutation(jax.random.fold_in(own_key, 1), count)
    favour = sequence
    for power in range(3):
        favour = favour * favour // count
    favour = favour * lift // count
    lots = jax.random.randint(jax.random.fold_in(own_key, 2), (rows, count), 0, 4096) + favour
    fixed_rows = jax.random.permutation(jax.random.fold_in(own_key, 3), rows)[jnp.arange(count) % rows]
    lots = jnp.where(jnp.arange(rows)[:, None] == fixed_rows[None, :], 1 << 14, lots)
    score = lots * count + jnp.arange(count)
    return lax.top_k(score.astype(jnp.int32), top)[1].astype(jnp.int32)


def assign_block(own_key, own, number, rows, number_of, top, most, slope):
    sequence = jax.random.permutation(own_key, number_of)
    packed, usual = shares(number_of, rows * top, most, slope, True), shares(number_of, rows * top, most, slope, False)
    places = jnp.arange(number_of)

    def named(sizes, offset_by):
        used = int((sizes > 0).sum())
        fixed = max(1, used // 4)
        moved = fixed + (places - fixed + offset_by * (used - fixed)) % max(1, number_of - fixed)
        return jnp.zeros((number_of,), jnp.int32).at[sequence[jnp.where(places < fixed, places, moved)]].set(jnp.asarray(sizes, jnp.int32))

    sizes = jnp.where(number % 4 == 0, named(packed, number // 4), named(usual, number - number // 4 - 1))
    mixed = jax.random.permutation(jax.random.fold_in(own, 3), number_of)
    source_of, taker = mixed[0:number_of // 2 * 2:2], mixed[1:number_of // 2 * 2:2]
    slack = jnp.minimum(sizes[source_of] - 1, most - sizes[taker]) // 2
    slack = jnp.where((source_of == sequence[0]) | (taker == sequence[0]) | (sizes[taker] == 0), 0, jnp.maximum(slack, 0))
    moved = jax.random.randint(jax.random.fold_in(own, 4), (number_of // 2,), 0, 1 << 20) % (slack + 1)
    sizes = sizes.at[source_of].add(-moved).at[taker].add(moved)
    labels = jnp.searchsorted(jnp.cumsum(sizes), jnp.arange(rows * top), side="right").astype(jnp.int32)
    grid = labels.reshape(top, rows).T
    grid = grid[jax.random.permutation(jax.random.fold_in(own, 1), rows)]
    offset_by = jax.random.randint(jax.random.fold_in(own, 2), (rows, 1), 0, top)
    return jnp.take_along_axis(grid, (jnp.arange(top)[None, :] + offset_by) % top, axis=1)


def shares(count, total, limit, lean, full):
    loads = [(1 << 20) // math.isqrt(grade ** lean) + 1 for grade in range(1, count + 1)]
    largest = limit if full else min(limit, max(-(-total // count), total * loads[0] // sum(loads)))
    least = 1 if total - largest >= count - 1 else 0
    counts, spare = [largest] + [least] * (count - 1), total - largest - least * (count - 1)
    while spare > 0:
        movable = [i for i in range(1, count) if counts[i] < largest] or [i for i in range(1, count) if counts[i] < limit]
        mass, remaining = sum([loads[i] for i in movable]), spare
        for i in movable:
            extra = min(limit - counts[i], max(1, remaining * loads[i] // mass), spare)
            counts[i] = counts[i] + extra
            spare = spare - extra
    return np.array(counts)


def noise(stream_key, extent, scale, reach, pieces=(), kind=jnp.bfloat16):
    result = jax.random.normal(stream_key, extent, jnp.float32) * scale
    if len(pieces) > 0:
        result = block_levels(stream_key, extent, pieces, -0.22, 0.18) * result
    return jnp.clip(result, min=-reach, max=reach).astype(kind)


def setup_inputs(seed: int = 0) -> dict:
    key_list = jax.random.split(jax.random.key(seed), 7)
    points = noise(key_list[0], (POINTS, D), 2.0, 12.0, ((0, 32),))
    block_rows = place_ends(jax.random.randint(key_list[1], (BLOCKS,), 1, BLOCK + 1), jax.random.fold_in(key_list[1], 1), 1, BLOCK).astype(jnp.int32)
    block_owner_keys = jax.random.split(jax.random.fold_in(key_list[2], 1), BLOCKS // (P_DEV // BLOCK))
    block_owner_turns = jax.random.permutation(jax.random.fold_in(key_list[2], 3), BLOCKS // (P_DEV // BLOCK))
    block_owner = jax.vmap(lambda own, number: assign_block(jax.random.fold_in(key_list[2], 2), own, number, P_DEV // BLOCK, DEVICES, 1, SLOTS, 2))(block_owner_keys, block_owner_turns).reshape((BLOCKS, 1))
    block_local = place_ends(jax.random.randint(key_list[3], (BLOCKS,), 0, K1_DEV), jax.random.fold_in(key_list[3], 1), 0, K1_DEV - 1).astype(jnp.int32)
    assign_mid = picks_of(key_list[4], K1, K2, 1, 0)
    assign_top = picks_of(key_list[5], K2, K3, 1, 0)
    return dict(points=points, block_rows=block_rows, block_owner=block_owner, block_local=block_local, assign_mid=assign_mid, assign_top=assign_top)


def reference(points, block_rows, block_owner, block_local, assign_mid, assign_top):
    feature_width = points.shape[1]
    block_count = P_DEV // BLOCK
    position = lax.broadcasted_iota(jnp.int32, (DEVICES, block_count, BLOCK), 2)
    live_rows = (position < block_rows.reshape(DEVICES, block_count, 1)).astype(jnp.float32)
    grouped = points.reshape(DEVICES, block_count, BLOCK, feature_width)

    def block_total(pair):
        masks, values = pair
        return jnp.einsum("bp,bpd->bd", masks, values.astype(jnp.float32))

    block_sums = lax.map(block_total, (live_rows, grouped)).reshape(DEVICES * block_count, feature_width)
    cluster = (block_owner[:, 0] * K1_DEV + block_local).astype(jnp.int32)
    level1_sums = jax.ops.segment_sum(block_sums, cluster, num_segments=K1)
    level1_counts = jax.ops.segment_sum(block_rows.astype(jnp.float32), cluster, num_segments=K1)
    level1 = level1_sums / jnp.maximum(level1_counts, 1.0)[:, None]
    rounded = level1.astype(jnp.bfloat16)
    widened = rounded.astype(jnp.float32)
    half_norm = 0.5 * jnp.sum(widened * widened, axis=1)
    live_points = live_rows.reshape(DEVICES, P_DEV)
    shard_points = points.reshape(DEVICES, P_DEV, feature_width)

    def scoring(pair):
        values, masks = pair
        product = jnp.dot(values, rounded.T, preferred_element_type=jnp.float32)
        return jnp.max(product - half_norm[None, :], axis=1) * masks

    best = lax.map(scoring, (shard_points, live_points)).reshape(DEVICES * P_DEV)
    mid_ids = assign_mid[:, 0].astype(jnp.int32)
    mid_counts = jax.ops.segment_sum(jnp.ones((K1,), jnp.float32), mid_ids, num_segments=K2)
    level2 = jax.ops.segment_sum(level1, mid_ids, num_segments=K2) / mid_counts[:, None]
    top_ids = assign_top[:, 0].astype(jnp.int32)
    top_counts = jax.ops.segment_sum(jnp.ones((K2,), jnp.float32), top_ids, num_segments=K3)
    level3 = jax.ops.segment_sum(level2, top_ids, num_segments=K3) / top_counts[:, None]
    return (level1, best, level2, level3)
```

```python
import functools

import jax
import jax.numpy as jnp
from jax import lax
from jax.experimental import pallas as pl
from jax.experimental.pallas import tpu as pltpu
from jax.sharding import PartitionSpec as P

SLOTS = 2
K1_DEV = 8
K3 = 256
CHUNK = 32
LANES = 128
TILE = 1024
ALL = ("dp", "group")


def sums_kernel(
    rows_hbm, owner_hbm, local_hbm, points_ref, out_ref, live_ref, parts, rows_ref, owner_ref, local_ref, taken, sems, small,
    *, blocks, block_len
):
    lines, _, width = out_ref.shape
    depth = width - LANES
    pieces = block_len // CHUNK

    def copy(g, n):
        rows = pl.ds(pl.multiple_of(g * block_len, block_len), n * CHUNK)
        return pltpu.make_async_copy(points_ref.at[rows, :], live_ref.at[rows, :], sems.at[g])

    def issue(g, carry):
        n = (rows_ref[g] + CHUNK - 1) // CHUNK
        for c in range(1, pieces + 1):

            @pl.when(n == c)
            def _():
                copy(g, c).start()

        return carry

    scalars = [
        pltpu.make_async_copy(rows_hbm, rows_ref, small.at[0]),
        pltpu.make_async_copy(owner_hbm, owner_ref, small.at[1]),
        pltpu.make_async_copy(local_hbm, local_ref, small.at[2]),
    ]
    for c in scalars:
        c.start()
    scalars[0].wait()
    lax.fori_loop(0, blocks, issue, 0)
    for c in scalars[1:]:
        c.wait()

    def clear(d, carry):
        taken[d] = 0
        return carry

    lax.fori_loop(0, lines // SLOTS, clear, 0)
    if lines > blocks:
        parts[...] = jnp.zeros_like(parts)
    row_index = lax.broadcasted_iota(jnp.int32, (CHUNK, depth), 0)

    def fold(values):
        return jnp.sum(values.astype(jnp.float32).reshape(-1, 8, depth), axis=0)

    def block(g, carry):
        rows = rows_ref[g]
        owner = owner_ref[g]
        slot = taken[owner]
        taken[owner] = slot + 1
        place = pl.multiple_of((owner * SLOTS + slot) * 8, 8)
        n = (rows + CHUNK - 1) // CHUNK
        code = (rows * K1_DEV + local_ref[g]).astype(jnp.float32) * (1.0 / 8)
        parts[depth // LANES, pl.ds(place, 8), :] = jnp.full((8, LANES), code, jnp.float32)
        for c in range(1, pieces + 1):

            @pl.when(n == c)
            def _():
                copy(g, c).wait()
                start = pl.multiple_of(g * block_len, block_len)
                tail = live_ref[pl.ds(start + (c - 1) * CHUNK, CHUNK), :].astype(jnp.float32)
                total = fold(jnp.where(row_index < rows - (c - 1) * CHUNK, tail, 0.0))
                if c > 1:
                    total = total + fold(live_ref[pl.ds(start, (c - 1) * CHUNK), :])
                for j in range(depth // LANES):
                    parts[j, pl.ds(place, 8), :] = total[:, j * LANES : (j + 1) * LANES]

        return carry

    lax.fori_loop(0, blocks, block, 0)
    for i in range(0, lines, 8):
        for j in range(width // LANES):
            lines_of = [parts[j, pl.ds(i * 8 + r, 8, stride=8), :] for r in range(8)]
            while len(lines_of) > 1:
                lines_of = [a + b for a, b in zip(lines_of[::2], lines_of[1::2])]
            out_ref[pl.ds(i, 8), 0, pl.ds(j * LANES, LANES)] = lines_of[0]


def power_of(exponent, bits=7):
    scale = jnp.ones_like(exponent)
    left = exponent
    for b in reversed(range(bits)):
        has = left >= float(1 << b)
        half = float(2.0 ** (1 << b)) if b < bits - 1 else float(2.0**64)
        scale = jnp.where(has, scale * half, scale)
        left = jnp.where(has, left - float(1 << b), left)
    return scale


def level1_kernel(got_ref, mid_ref, top_ref, level1_ref, send_ref, *, parts):
    lines, _, width = got_ref.shape
    depth = width - LANES
    local = lax.broadcasted_iota(jnp.int32, (K1_DEV, LANES), 0).astype(jnp.float32)
    sums = jnp.zeros((K1_DEV, depth), jnp.float32)
    counts = jnp.zeros((K1_DEV, LANES), jnp.float32)
    for i in range(lines):
        line = got_ref[i]
        code = jnp.broadcast_to(line[:, depth:], (K1_DEV, LANES))
        count = jnp.floor(code * (1.0 / K1_DEV))
        mine = (code - count * K1_DEV) == local
        counts = counts + jnp.where(mine, count, 0.0)
        keep = jnp.concatenate([mine] * (depth // LANES), axis=1)
        sums = sums + jnp.where(keep, jnp.broadcast_to(line[:, :depth], (K1_DEV, depth)), 0.0)
    denominator = jnp.concatenate([jnp.maximum(counts, 1.0)] * (depth // LANES), axis=1)
    level1 = sums / denominator
    level1_ref[...] = level1
    top_value = jnp.max(jnp.abs(level1), axis=1, keepdims=True)
    scale = jnp.ones_like(top_value)
    exponent = jnp.zeros_like(top_value)
    for b in (32, 32, 32, 16, 8, 4, 2, 1):
        grown = top_value * scale * float(2.0**b)
        fits = (grown <= 64.0) & (exponent + b <= 100.0)
        scale = jnp.where(fits, scale * float(2.0**b), scale)
        exponent = jnp.where(fits, exponent + b, exponent)
    value = level1 * scale
    split = value * 8193.0
    coarse = split - (split - value)
    rounded = value.astype(jnp.bfloat16).astype(jnp.float32)
    kept = coarse.astype(jnp.bfloat16).astype(jnp.float32) == rounded
    coded = jnp.where(kept, coarse, coarse + (rounded - coarse) * 0.25)
    send_ref[:, pl.ds(0, depth)] = coded
    lane = lax.broadcasted_iota(jnp.int32, (K1_DEV, LANES), 1)
    extra = jnp.where(lane == 0, exponent, 0.0)
    extra = jnp.where(lane == 1, mid_ref[...].astype(jnp.float32), extra)
    for k in range(parts):
        extra = jnp.where(lane == 2 + k, top_ref[:, k : k + 1].astype(jnp.float32), extra)
    send_ref[:, pl.ds(depth, LANES)] = extra


def last_kernel(
    rows_ref, place_ref, points_ref, gathered_ref, best_ref, level2_ref, level3_ref, live_ref, high, low, half_norm, two, three,
    sems, fetched,
    *, origins, group, parts
):
    count, width = gathered_ref.shape
    depth = width - LANES
    second = group * K1_DEV * parts
    block_len = LANES

    def fetch(g, n):
        rows = pl.ds(pl.multiple_of(g * block_len, block_len), n * CHUNK)
        return pltpu.make_async_copy(points_ref.at[rows, :], live_ref.at[rows, :], fetched.at[g])

    def each(g, act):
        n = (rows_ref[g] + CHUNK - 1) // CHUNK
        for c in range(1, block_len // CHUNK + 1):

            @pl.when(n == c)
            def _():
                act(fetch(g, c))

    def issue(g, carry):
        each(g, lambda copy: copy.start())
        return carry

    lax.fori_loop(0, rows_ref.shape[0], issue, 0)
    extra = gathered_ref[:, pl.ds(depth, LANES)]
    value = gathered_ref[:, pl.ds(0, depth)] * (1.0 / power_of(extra[:, 0:1]))
    upper = value.astype(jnp.bfloat16)
    wide = upper.astype(jnp.float32)
    high[...] = upper
    low[...] = (value - wide).astype(jnp.bfloat16)
    half_norm[...] = 0.5 * jnp.sum(wide * wide, axis=1, keepdims=True)

    def total(chooser, upper, lower):
        dims = (((0,), (0,)), ((), ()))
        a = lax.dot_general(chooser, upper, dims, preferred_element_type=jnp.float32)
        b = lax.dot_general(chooser, lower, dims, preferred_element_type=jnp.float32)
        ones = jnp.ones((chooser.shape[0], LANES), jnp.bfloat16)
        n = lax.dot_general(chooser, ones, dims, preferred_element_type=jnp.float32)
        return (a + b) / n[:, 0:1]

    mid = extra[:, 1:2].astype(jnp.int32)
    size = K1_DEV * parts
    owner = (mid // size) ^ place_ref[0]
    inner = mid % size
    index = (inner // K1_DEV) * (group * K1_DEV) + owner * K1_DEV + inner % K1_DEV
    chooser = (index == lax.broadcasted_iota(jnp.int32, (count, second), 1)).astype(jnp.float32).astype(jnp.bfloat16)
    level2 = total(chooser, high[...], low[...])
    for k in range(parts):
        two[pl.ds(k * K1_DEV, K1_DEV), :] = level2[k * group * K1_DEV : k * group * K1_DEV + K1_DEV, :]
    order = [origins.index((0, q)) for q in range(group)]
    tops = [extra[p * K1_DEV : (p + 1) * K1_DEV, 2 + k : 3 + k] for k in range(parts) for p in order]
    top = jnp.concatenate(tops, axis=0).astype(jnp.int32)
    chooser = (top == lax.broadcasted_iota(jnp.int32, (second, K3), 1)).astype(jnp.float32).astype(jnp.bfloat16)
    upper = level2.astype(jnp.bfloat16)
    lower = (level2 - upper.astype(jnp.float32)).astype(jnp.bfloat16)
    three[...] = total(chooser, upper, lower)
    copies = [
        pltpu.make_async_copy(two, level2_ref, sems.at[0]),
        pltpu.make_async_copy(three, level3_ref, sems.at[1]),
    ]
    for c in copies:
        c.start()
    lane = lax.broadcasted_iota(jnp.int32, (1, LANES), 1)

    def scores(t, carry):
        for b in range(TILE // LANES):
            each(t * (TILE // LANES) + b, lambda copy: copy.wait())
        score = lax.dot_general(
            high[...],
            live_ref[pl.ds(pl.multiple_of(t * TILE, TILE), TILE), :],
            (((1,), (1,)), ((), ())),
            preferred_element_type=jnp.float32,
        )
        found = jnp.max(score - half_norm[...], axis=0, keepdims=True)
        for b in range(TILE // LANES):
            g = t * (TILE // LANES) + b
            best_ref[pl.ds(g, 1), :] = jnp.where(lane < rows_ref[g], found[:, b * LANES : (b + 1) * LANES], 0.0)
        return carry

    lax.fori_loop(0, live_ref.shape[0] // TILE, scores, 0)
    for c in copies:
        c.wait()


def gather(values, stages, devices):
    order = [0]
    for masks in stages:
        pieces = [values]
        for m in masks:
            pieces.append(lax.ppermute(values, ALL, [(i, i ^ m) for i in range(devices)]))
        values = jnp.concatenate(pieces, axis=0)
        order = [q ^ m for m in [0] + list(masks) for q in order]
    return values, order


def local(points, block_rows, block_owner, block_local, assign_mid, assign_top):
    dp, group = lax.axis_size("dp"), lax.axis_size("group")
    devices = dp * group
    rows, depth = points.shape
    blocks = block_rows.shape[0]
    parts = assign_top.shape[0] // K1_DEV
    width = depth + LANES
    smem = pl.BlockSpec(memory_space=pltpu.SMEM)
    vmem = pl.BlockSpec(memory_space=pltpu.VMEM)
    hbm = pl.BlockSpec(memory_space=pltpu.HBM)
    sums = pl.pallas_call(
        functools.partial(sums_kernel, blocks=blocks, block_len=rows // blocks),
        out_shape=jax.ShapeDtypeStruct((devices * SLOTS, 1, width), jnp.float32),
        in_specs=[hbm] * 4,
        out_specs=vmem,
        scratch_shapes=[
            pltpu.VMEM((rows, depth), jnp.bfloat16),
            pltpu.VMEM((width // LANES, devices * SLOTS * 8, LANES), jnp.float32),
            pltpu.SMEM((blocks,), jnp.int32),
            pltpu.SMEM((blocks,), jnp.int32),
            pltpu.SMEM((blocks,), jnp.int32),
            pltpu.SMEM((devices,), jnp.int32),
            pltpu.SemaphoreType.DMA((blocks,)),
            pltpu.SemaphoreType.DMA((3,)),
        ],
        compiler_params=pltpu.CompilerParams(vmem_limit_bytes=58 << 20),
        name="block_sums",
    )(block_rows, block_owner[:, 0], block_local, points)
    got = lax.all_to_all(sums, ALL, split_axis=0, concat_axis=0, tiled=True)
    level1, send = pl.pallas_call(
        functools.partial(level1_kernel, parts=parts),
        out_shape=(
            jax.ShapeDtypeStruct((K1_DEV, depth), jnp.float32),
            jax.ShapeDtypeStruct((K1_DEV, width), jnp.float32),
        ),
        in_specs=[vmem] * 3,
        out_specs=(vmem, vmem),
        compiler_params=pltpu.CompilerParams(vmem_limit_bytes=16 << 20),
        name="level1",
    )(got, assign_mid, assign_top.reshape(parts, K1_DEV).T)
    bits = [1 << b for b in reversed(range((devices - 1).bit_length()))]
    gathered, order = gather(send.astype(jnp.float16), [[b] for b in bits], devices)
    origins = [(q // group, q % group) for q in order]
    place = lax.axis_index("group").astype(jnp.int32).reshape(1)
    best, level2, level3 = pl.pallas_call(
        functools.partial(last_kernel, origins=origins, group=group, parts=parts),
        out_shape=(
            jax.ShapeDtypeStruct((blocks, LANES), jnp.float32),
            jax.ShapeDtypeStruct((K1_DEV * parts, depth), jnp.float32),
            jax.ShapeDtypeStruct((K3, depth), jnp.float32),
        ),
        in_specs=[smem, smem, hbm, vmem],
        out_specs=(vmem, pl.BlockSpec(memory_space=pl.ANY), pl.BlockSpec(memory_space=pl.ANY)),
        scratch_shapes=[
            pltpu.VMEM((rows, depth), jnp.bfloat16),
            pltpu.VMEM((devices * K1_DEV, depth), jnp.bfloat16),
            pltpu.VMEM((devices * K1_DEV, depth), jnp.bfloat16),
            pltpu.VMEM((devices * K1_DEV, 1), jnp.float32),
            pltpu.VMEM((K1_DEV * parts, depth), jnp.float32),
            pltpu.VMEM((K3, depth), jnp.float32),
            pltpu.SemaphoreType.DMA((2,)),
            pltpu.SemaphoreType.DMA((blocks,)),
        ],
        compiler_params=pltpu.CompilerParams(vmem_limit_bytes=58 << 20),
        name="scores",
    )(block_rows, place, points, gathered.astype(jnp.float32))
    return (level1, best.reshape(rows), level2, level3)


def solution(mesh):
    return jax.shard_map(
        local,
        mesh=mesh,
        in_specs=(
            P(("dp", "group"), None),
            P(("dp", "group")),
            P(("dp", "group"), None),
            P(("dp", "group")),
            P(("dp", "group"), None),
            P("group", None),
        ),
        out_specs=(P(("dp", "group"), None), P(("dp", "group")), P("group", None), P()),
        check_vma=False,
    )
```

```python
import functools

import jax
import jax.numpy as jnp
from jax import lax
from jax.experimental import pallas as pl
from jax.experimental.pallas import tpu as pltpu
from jax.sharding import PartitionSpec as P

SLOTS = 2
K1_DEV = 8
K3 = 256
CHUNK = 32
LANES = 128
TILE = 2048
ALL = ("dp", "group")


def sums_kernel(rows_hbm, owner_hbm, local_hbm, mid_hbm, top_hbm, points_ref, *refs, blocks, block_len, dp, group, parts):
    out_refs, (ids_ref, live_ref, partial, rows_ref, owner_ref, local_ref, mid_ref, top_ref, taken, sems, small) = (
        refs[:group],
        refs[group:],
    )
    each, width = out_refs[0].shape
    lines = each * group
    depth = width - LANES
    pieces = block_len // CHUNK

    def copy(g, n):
        rows = pl.ds(pl.multiple_of(g * block_len, block_len), n * CHUNK)
        return pltpu.make_async_copy(points_ref.at[rows, :], live_ref.at[rows, :], sems.at[g])

    def issue(g, carry):
        n = (rows_ref[g] + CHUNK - 1) // CHUNK
        for c in range(1, pieces + 1):

            @pl.when(n == c)
            def _():
                copy(g, c).start()

        return carry

    scalars = [
        pltpu.make_async_copy(rows_hbm, rows_ref, small.at[0]),
        pltpu.make_async_copy(owner_hbm, owner_ref, small.at[1]),
        pltpu.make_async_copy(local_hbm, local_ref, small.at[2]),
        pltpu.make_async_copy(mid_hbm, mid_ref, small.at[3]),
        pltpu.make_async_copy(top_hbm, top_ref, small.at[4]),
    ]
    for c in scalars:
        c.start()
    scalars[0].wait()
    lax.fori_loop(0, blocks, issue, 0)
    for c in scalars[1:]:
        c.wait()

    def clear(d, carry):
        taken[d] = 0
        return carry

    lax.fori_loop(0, lines // SLOTS, clear, 0)
    if lines > blocks:
        partial[...] = jnp.zeros_like(partial)
    row_index = lax.broadcasted_iota(jnp.int32, (CHUNK, depth), 0)
    mine, here = lax.axis_index("dp"), lax.axis_index("group")
    sub = lax.broadcasted_iota(jnp.int32, (K1_DEV, LANES), 0)
    lane = lax.broadcasted_iota(jnp.int32, (K1_DEV, LANES), 1)
    ids = jnp.zeros((K1_DEV, LANES), jnp.int32)
    for r in range(K1_DEV):
        ids = jnp.where((sub == r) & (lane == 3), mid_ref[r], ids)
        for p in range(parts):
            ids = jnp.where((sub == r) & (lane == 4 + p), top_ref[p * K1_DEV + r], ids)
    ids_ref[...] = ids.astype(jnp.float32)

    def fold(values):
        return jnp.sum(values.astype(jnp.float32).reshape(-1, 8, depth), axis=0)

    def block(g, carry):
        rows = rows_ref[g]
        owner = owner_ref[g]
        slot = taken[owner]
        taken[owner] = slot + 1
        column = (owner // group) ^ mine
        place = pl.multiple_of(((((owner % group) ^ here) * dp + column) * SLOTS + slot) * 8, 8)
        n = (rows + CHUNK - 1) // CHUNK
        code = (rows * K1_DEV + local_ref[g]).astype(jnp.float32) * (1.0 / 8)
        partial[depth // LANES, pl.ds(place, 8), :] = jnp.full((8, LANES), code, jnp.float32)
        for c in range(1, pieces + 1):

            @pl.when(n == c)
            def _():
                copy(g, c).wait()
                start = pl.multiple_of(g * block_len, block_len)
                tail = live_ref[pl.ds(start + (c - 1) * CHUNK, CHUNK), :].astype(jnp.float32)
                total = fold(jnp.where(row_index < rows - (c - 1) * CHUNK, tail, 0.0))
                if c > 1:
                    total = total + fold(live_ref[pl.ds(start, (c - 1) * CHUNK), :])
                for j in range(depth // LANES):
                    partial[j, pl.ds(place, 8), :] = total[:, j * LANES : (j + 1) * LANES]

        return carry

    lax.fori_loop(0, blocks, block, 0)
    for i in range(0, lines, 8):
        for j in range(width // LANES):
            lines_of = [partial[j, pl.ds(i * 8 + r, 8, stride=8), :] for r in range(8)]
            while len(lines_of) > 1:
                lines_of = [a + b for a, b in zip(lines_of[::2], lines_of[1::2])]
            out_refs[i // each][pl.ds(i % each, 8), pl.ds(j * LANES, LANES)] = lines_of[0]


def power_of(exponent):
    scale = jnp.full_like(exponent, 0.0625)
    left = exponent + 4.0
    for b in (64, 32, 16, 8, 4, 2, 1):
        has = left >= float(b)
        scale = jnp.where(has, scale * float(2.0**b), scale)
        left = jnp.where(has, left - float(b), left)
    return scale


def fitted(values):
    top_value = jnp.max(jnp.abs(values), axis=1, keepdims=True)
    shrink = top_value > 16384.0
    scale = jnp.where(shrink, 0.0625, jnp.ones_like(top_value))
    exponent = jnp.where(shrink, -4.0, jnp.zeros_like(top_value))
    for b in (32, 32, 32, 16, 8, 4, 2, 1):
        fits = (top_value * scale * float(2.0**b) <= 16384.0) & (exponent + b <= 100.0)
        scale = jnp.where(fits, scale * float(2.0**b), scale)
        exponent = jnp.where(fits, exponent + b, exponent)
    value = values * scale
    split = value * 8193.0
    return value, split - (split - value), exponent


def partial_kernel(*refs, dp, group):
    got_refs, (ids_ref, send_ref) = refs[:group], refs[group:]
    width = send_ref.shape[1]
    depth = width - LANES
    local = lax.broadcasted_iota(jnp.int32, (K1_DEV, LANES), 0).astype(jnp.float32)
    lane = lax.broadcasted_iota(jnp.int32, (K1_DEV, LANES), 1)
    for r in range(dp):
        sums = jnp.zeros((K1_DEV, depth), jnp.float32)
        counts = jnp.zeros((K1_DEV, LANES), jnp.float32)
        for g in range(group):
            for t in range(SLOTS):
                line = got_refs[g][pl.ds(r * SLOTS + t, 1), :]
                code = jnp.broadcast_to(line[:, depth:], (K1_DEV, LANES))
                count = jnp.floor(code * (1.0 / K1_DEV))
                mine = (code - count * K1_DEV) == local
                counts = counts + jnp.where(mine, count, 0.0)
                keep = jnp.concatenate([mine] * (depth // LANES), axis=1)
                sums = sums + jnp.where(keep, jnp.broadcast_to(line[:, :depth], (K1_DEV, depth)), 0.0)
        _, coded, exponent = fitted(sums)
        send_ref[pl.ds(r * K1_DEV, K1_DEV), pl.ds(0, depth)] = coded
        many = jnp.floor(counts * (1.0 / 1024))
        extra = ids_ref[...] if r == 0 else jnp.zeros((K1_DEV, LANES), jnp.float32)
        extra = jnp.where(lane == 0, exponent, jnp.where(lane == 1, counts - many * 1024, jnp.where(lane == 2, many, extra)))
        send_ref[pl.ds(r * K1_DEV, K1_DEV), pl.ds(depth, LANES)] = extra


def level1_kernel(*refs, dp, parts):
    pieces, (ids_ref, level1_ref, send_ref) = refs[:dp], refs[dp:]
    width = send_ref.shape[1]
    depth = width - LANES
    lane = lax.broadcasted_iota(jnp.int32, (K1_DEV, LANES), 1)
    for r in range(dp):
        terms, counts = [], []
        for q in range(dp):
            rows = pl.ds((r ^ q) * K1_DEV, K1_DEV)
            extra = pieces[q][rows, pl.ds(depth, LANES)]
            terms.append(pieces[q][rows, pl.ds(0, depth)] * (1.0 / power_of(extra[:, 0:1])))
            counts.append(extra[:, 1:2] + extra[:, 2:3] * 1024.0)
        while len(terms) > 1:
            terms = [a + b for a, b in zip(terms[::2], terms[1::2])]
            counts = [a + b for a, b in zip(counts[::2], counts[1::2])]
        level1 = terms[0] / jnp.maximum(counts[0], 1.0)
        if r == 0:
            level1_ref[...] = level1
        value, coarse, exponent = fitted(level1)
        rounded = value.astype(jnp.bfloat16).astype(jnp.float32)
        kept = coarse.astype(jnp.bfloat16).astype(jnp.float32) == rounded
        coded = jnp.where(kept, coarse, coarse + (rounded - coarse) * 0.25)
        send_ref[pl.ds(r * K1_DEV, K1_DEV), pl.ds(0, depth)] = coded
        mid = pieces[r][pl.ds(0, K1_DEV), pl.ds(depth, LANES)][:, 3:4]
        extra = jnp.where(lane == 0, exponent, jnp.where(lane == 1, mid, 0.0))
        for k in range(parts):
            extra = jnp.where(lane == 2 + k, ids_ref[:, 4 + k : 5 + k], extra)
        send_ref[pl.ds(r * K1_DEV, K1_DEV), pl.ds(depth, LANES)] = extra


def last_kernel(
    rows_ref, live_ref, *refs, origins, group, parts, pieces, tile
):
    gathered, (best_ref, level2_ref, level3_ref, high, low, half_norm, two, three, sems) = refs[:pieces], refs[pieces:]
    size, width = gathered[0].shape
    count = size * pieces
    depth = width - LANES
    second = group * K1_DEV * parts
    extra = jnp.concatenate([ref[:, pl.ds(depth, LANES)] for ref in gathered], axis=0)
    unscale = 1.0 / power_of(extra[:, 0:1])
    for i, ref in enumerate(gathered):
        rows = pl.ds(i * size, size)
        value = ref[:, pl.ds(0, depth)] * unscale[i * size : (i + 1) * size]
        upper = value.astype(jnp.bfloat16)
        wide = upper.astype(jnp.float32)
        high[rows, :] = upper
        low[rows, :] = (value - wide).astype(jnp.bfloat16)
        half_norm[rows, :] = 0.5 * jnp.sum(wide * wide, axis=1, keepdims=True)

    def total(chooser, upper, lower):
        dims = (((0,), (0,)), ((), ()))
        a = lax.dot_general(chooser, upper, dims, preferred_element_type=jnp.float32)
        b = lax.dot_general(chooser, lower, dims, preferred_element_type=jnp.float32)
        ones = jnp.ones((chooser.shape[0], LANES), jnp.bfloat16)
        n = lax.dot_general(chooser, ones, dims, preferred_element_type=jnp.float32)
        return (a + b) / n[:, 0:1]

    mid = extra[:, 1:2].astype(jnp.int32)
    size = K1_DEV * parts
    owner = (mid // size) ^ lax.axis_index("group")
    inner = mid % size
    index = (inner // K1_DEV) * (group * K1_DEV) + owner * K1_DEV + inner % K1_DEV
    chooser = (index == lax.broadcasted_iota(jnp.int32, (count, second), 1)).astype(jnp.float32).astype(jnp.bfloat16)
    level2 = total(chooser, high[...], low[...])
    for k in range(parts):
        two[pl.ds(k * K1_DEV, K1_DEV), :] = level2[k * group * K1_DEV : k * group * K1_DEV + K1_DEV, :]
    order = [origins.index((0, q)) for q in range(group)]
    tops = [extra[p * K1_DEV : (p + 1) * K1_DEV, 2 + k : 3 + k] for k in range(parts) for p in order]
    top = jnp.concatenate(tops, axis=0).astype(jnp.int32)
    chooser = (top == lax.broadcasted_iota(jnp.int32, (second, K3), 1)).astype(jnp.float32).astype(jnp.bfloat16)
    upper = level2.astype(jnp.bfloat16)
    lower = (level2 - upper.astype(jnp.float32)).astype(jnp.bfloat16)
    three[...] = total(chooser, upper, lower)
    copies = [
        pltpu.make_async_copy(two, level2_ref, sems.at[0]),
        pltpu.make_async_copy(three, level3_ref, sems.at[1]),
    ]
    for c in copies:
        c.start()
    lane = lax.broadcasted_iota(jnp.int32, (1, LANES), 1)

    def scores(t, carry):
        score = lax.dot_general(
            high[...],
            live_ref[pl.ds(pl.multiple_of(t * tile, tile), tile), :],
            (((1,), (1,)), ((), ())),
            preferred_element_type=jnp.float32,
        )
        found = jnp.max(score - half_norm[...], axis=0, keepdims=True)
        for b in range(tile // LANES):
            g = t * (tile // LANES) + b
            best_ref[pl.ds(g, 1), :] = jnp.where(lane < rows_ref[g], found[:, b * LANES : (b + 1) * LANES], 0.0)
        return carry

    lax.fori_loop(0, live_ref.shape[0] // tile, scores, 0)
    for c in copies:
        c.wait()


def swap(values, mask, devices):
    return lax.ppermute(values, ALL, [(i, i ^ mask) for i in range(devices)])


def gather(values, group, devices):
    order = [0]
    bit = group
    while bit > 1:
        step = min(4, bit)
        if bit == 8:
            step = 4
        bit //= step
        masks = [bit * q for q in range(1, step)]
        pieces = [values] + [swap(values, m, devices) for m in masks]
        order = [q ^ m for m in [0] + masks for q in order]
        if bit > 1:
            values = jnp.concatenate(pieces, axis=0)
    return pieces, order


def local(points, block_rows, block_owner, block_local, assign_mid, assign_top):
    dp, group = lax.axis_size("dp"), lax.axis_size("group")
    devices = dp * group
    rows, depth = points.shape
    blocks = block_rows.shape[0]
    parts = assign_top.shape[0] // K1_DEV
    width = depth + LANES
    smem = pl.BlockSpec(memory_space=pltpu.SMEM)
    vmem = pl.BlockSpec(memory_space=pltpu.VMEM)
    hbm = pl.BlockSpec(memory_space=pltpu.HBM)
    pieces = pl.pallas_call(
        functools.partial(sums_kernel, blocks=blocks, block_len=rows // blocks, dp=dp, group=group, parts=parts),
        out_shape=tuple(pltpu.VMEM((dp * SLOTS, width), jnp.float32) for _ in range(group))
        + (pltpu.VMEM((K1_DEV, LANES), jnp.float32), pltpu.VMEM((rows, depth), jnp.bfloat16)),
        in_specs=[hbm] * 6,
        out_specs=(vmem,) * (group + 2),
        scratch_shapes=[
            pltpu.VMEM((width // LANES, devices * SLOTS * 8, LANES), jnp.float32),
            pltpu.SMEM((blocks,), jnp.int32),
            pltpu.SMEM((blocks,), jnp.int32),
            pltpu.SMEM((blocks,), jnp.int32),
            pltpu.SMEM((K1_DEV,), jnp.int32),
            pltpu.SMEM((K1_DEV * parts,), jnp.int32),
            pltpu.SMEM((devices,), jnp.int32),
            pltpu.SemaphoreType.DMA((blocks,)),
            pltpu.SemaphoreType.DMA((5,)),
        ],
        compiler_params=pltpu.CompilerParams(vmem_limit_bytes=40 << 20),
        name="block_sums",
    )(block_rows, block_owner[:, 0], block_local, assign_mid[:, 0], assign_top[:, 0], points)
    ids, live = pieces[group:]
    got = [pieces[0]] + [swap(pieces[q], q, devices) for q in range(1, group)]
    own = pl.pallas_call(
        functools.partial(partial_kernel, dp=dp, group=group),
        out_shape=pltpu.VMEM((dp * K1_DEV, width), jnp.float32),
        in_specs=[vmem] * (group + 1),
        out_specs=vmem,
        compiler_params=pltpu.CompilerParams(vmem_limit_bytes=16 << 20),
        name="partial_sums",
    )(*got, ids)
    half = own.astype(jnp.float16)
    others = [swap(half, q * group, devices).astype(jnp.float32) for q in range(1, dp)]
    level1, send = pl.pallas_call(
        functools.partial(level1_kernel, dp=dp, parts=parts),
        out_shape=(
            jax.ShapeDtypeStruct((K1_DEV, depth), jnp.float32),
            pltpu.VMEM((dp * K1_DEV, width), jnp.float32),
        ),
        in_specs=[vmem] * (dp + 1),
        out_specs=(vmem, vmem),
        compiler_params=pltpu.CompilerParams(vmem_limit_bytes=16 << 20),
        name="level1",
    )(own, *others, ids)
    gathered, order = gather(send.astype(jnp.float16), group, devices)
    origins = [(r, q) for q in order for r in range(dp)]
    best, level2, level3 = pl.pallas_call(
        functools.partial(
            last_kernel, origins=origins, group=group, parts=parts, pieces=len(gathered), tile=min(TILE, TILE * K3 // (devices * K1_DEV))
        ),
        out_shape=(
            jax.ShapeDtypeStruct((blocks, LANES), jnp.float32),
            jax.ShapeDtypeStruct((K1_DEV * parts, depth), jnp.float32),
            jax.ShapeDtypeStruct((K3, depth), jnp.float32),
        ),
        in_specs=[smem] + [vmem] * (1 + len(gathered)),
        out_specs=(vmem, pl.BlockSpec(memory_space=pl.ANY), pl.BlockSpec(memory_space=pl.ANY)),
        scratch_shapes=[
            pltpu.VMEM((devices * K1_DEV, depth), jnp.bfloat16),
            pltpu.VMEM((devices * K1_DEV, depth), jnp.bfloat16),
            pltpu.VMEM((devices * K1_DEV, 1), jnp.float32),
            pltpu.VMEM((K1_DEV * parts, depth), jnp.float32),
            pltpu.VMEM((K3, depth), jnp.float32),
            pltpu.SemaphoreType.DMA((2,)),
        ],
        compiler_params=pltpu.CompilerParams(vmem_limit_bytes=40 << 20),
        name="scores",
    )(block_rows, pltpu.with_memory_space_constraint(live, pltpu.VMEM), *[g.astype(jnp.float32) for g in gathered])
    return (level1, best.reshape(rows), level2, level3)


def solution(mesh):
    return jax.shard_map(
        local,
        mesh=mesh,
        in_specs=(
            P(("dp", "group"), None),
            P(("dp", "group")),
            P(("dp", "group"), None),
            P(("dp", "group")),
            P(("dp", "group"), None),
            P("group", None),
        ),
        out_specs=(P(("dp", "group"), None), P(("dp", "group")), P("group", None), P()),
        check_vma=False,
    )
```

```python
import functools

import jax
import jax.numpy as jnp
from jax import lax
from jax.experimental import pallas as pl
from jax.experimental.pallas import tpu as pltpu
from jax.sharding import PartitionSpec as P

SLOTS = 2
K1_DEV = 8
K3 = 256
CHUNK = 32
LANES = 128
TILE = 4096
ALL = ("dp", "group")


def sums_kernel(rows_hbm, owner_hbm, local_hbm, mid_hbm, top_hbm, points_ref, *refs, blocks, block_len, dp, group, parts):
    out_refs, (ids_ref, live_ref, partial, rows_ref, owner_ref, local_ref, mid_ref, top_ref, taken, sems, small) = (
        refs[:group],
        refs[group:],
    )
    each, width = out_refs[0].shape
    lines = each * group
    depth = width - LANES
    pieces = block_len // CHUNK

    def copy(g, n):
        rows = pl.ds(pl.multiple_of(g * block_len, block_len), n * CHUNK)
        return pltpu.make_async_copy(points_ref.at[rows, :], live_ref.at[rows, :], sems.at[g])

    def issue(g, carry):
        n = (rows_ref[g] + CHUNK - 1) // CHUNK
        for c in range(1, pieces + 1):

            @pl.when(n == c)
            def _():
                copy(g, c).start()

        return carry

    scalars = [
        pltpu.make_async_copy(rows_hbm, rows_ref, small.at[0]),
        pltpu.make_async_copy(owner_hbm, owner_ref, small.at[1]),
        pltpu.make_async_copy(local_hbm, local_ref, small.at[2]),
        pltpu.make_async_copy(mid_hbm, mid_ref, small.at[3]),
        pltpu.make_async_copy(top_hbm, top_ref, small.at[4]),
    ]
    for c in scalars:
        c.start()
    scalars[0].wait()
    lax.fori_loop(0, blocks, issue, 0)
    for c in scalars[1:]:
        c.wait()

    def clear(d, carry):
        taken[d] = 0
        return carry

    lax.fori_loop(0, lines // SLOTS, clear, 0)
    if lines > blocks:
        partial[...] = jnp.zeros_like(partial)
    row_index = lax.broadcasted_iota(jnp.int32, (CHUNK, depth), 0)
    mine, here = lax.axis_index("dp"), lax.axis_index("group")
    sub = lax.broadcasted_iota(jnp.int32, (K1_DEV, LANES), 0)
    lane = lax.broadcasted_iota(jnp.int32, (K1_DEV, LANES), 1)
    ids = jnp.zeros((K1_DEV, LANES), jnp.int32)
    for r in range(K1_DEV):
        ids = jnp.where((sub == r) & (lane == 3), mid_ref[r], ids)
        for p in range(parts):
            ids = jnp.where((sub == r) & (lane == 4 + p), top_ref[p * K1_DEV + r], ids)
    ids_ref[...] = ids.astype(jnp.float32)

    def fold(values):
        return jnp.sum(values.astype(jnp.float32).reshape(-1, 8, depth), axis=0)

    def block(g, carry):
        rows = rows_ref[g]
        owner = owner_ref[g]
        slot = taken[owner]
        taken[owner] = slot + 1
        column = (owner // group) ^ mine
        place = pl.multiple_of(((((owner % group) ^ here) * dp + column) * SLOTS + slot) * 8, 8)
        n = (rows + CHUNK - 1) // CHUNK
        code = (rows * K1_DEV + local_ref[g]).astype(jnp.float32) * (1.0 / 8)
        partial[depth // LANES, pl.ds(place, 8), :] = jnp.full((8, LANES), code, jnp.float32)
        for c in range(1, pieces + 1):

            @pl.when(n == c)
            def _():
                copy(g, c).wait()
                start = pl.multiple_of(g * block_len, block_len)
                tail = live_ref[pl.ds(start + (c - 1) * CHUNK, CHUNK), :].astype(jnp.float32)
                total = fold(jnp.where(row_index < rows - (c - 1) * CHUNK, tail, 0.0))
                if c > 1:
                    total = total + fold(live_ref[pl.ds(start, (c - 1) * CHUNK), :])
                for j in range(depth // LANES):
                    partial[j, pl.ds(place, 8), :] = total[:, j * LANES : (j + 1) * LANES]

        return carry

    lax.fori_loop(0, blocks, block, 0)
    for i in range(0, lines, 8):
        for j in range(width // LANES):
            lines_of = [partial[j, pl.ds(i * 8 + r, 8, stride=8), :] for r in range(8)]
            while len(lines_of) > 1:
                lines_of = [a + b for a, b in zip(lines_of[::2], lines_of[1::2])]
            out_refs[i // each][pl.ds(i % each, 8), pl.ds(j * LANES, LANES)] = lines_of[0]


def power_of(exponent):
    scale = jnp.full_like(exponent, 0.0625)
    left = exponent + 4.0
    for b in (64, 32, 16, 8, 4, 2, 1):
        has = left >= float(b)
        scale = jnp.where(has, scale * float(2.0**b), scale)
        left = jnp.where(has, left - float(b), left)
    return scale


def fitted(values):
    top_value = jnp.max(jnp.abs(values), axis=1, keepdims=True)
    shrink = top_value > 16384.0
    scale = jnp.where(shrink, 0.0625, jnp.ones_like(top_value))
    exponent = jnp.where(shrink, -4.0, jnp.zeros_like(top_value))
    for b in (32, 32, 32, 16, 8, 4, 2, 1):
        fits = (top_value * scale * float(2.0**b) <= 16384.0) & (exponent + b <= 100.0)
        scale = jnp.where(fits, scale * float(2.0**b), scale)
        exponent = jnp.where(fits, exponent + b, exponent)
    value = values * scale
    split = value * 8193.0
    return value, split - (split - value), exponent


def partial_kernel(*refs, dp, group):
    got_refs, (ids_ref, send_ref) = refs[:group], refs[group:]
    width = send_ref.shape[1]
    depth = width - LANES
    local = lax.broadcasted_iota(jnp.int32, (K1_DEV, LANES), 0).astype(jnp.float32)
    lane = lax.broadcasted_iota(jnp.int32, (K1_DEV, LANES), 1)
    for r in range(dp):
        sums = jnp.zeros((K1_DEV, depth), jnp.float32)
        counts = jnp.zeros((K1_DEV, LANES), jnp.float32)
        for g in range(group):
            for t in range(SLOTS):
                line = got_refs[g][pl.ds(r * SLOTS + t, 1), :]
                code = jnp.broadcast_to(line[:, depth:], (K1_DEV, LANES))
                count = jnp.floor(code * (1.0 / K1_DEV))
                mine = (code - count * K1_DEV) == local
                counts = counts + jnp.where(mine, count, 0.0)
                keep = jnp.concatenate([mine] * (depth // LANES), axis=1)
                sums = sums + jnp.where(keep, jnp.broadcast_to(line[:, :depth], (K1_DEV, depth)), 0.0)
        _, coded, exponent = fitted(sums)
        send_ref[pl.ds(r * K1_DEV, K1_DEV), pl.ds(0, depth)] = coded
        many = jnp.floor(counts * (1.0 / 1024))
        extra = ids_ref[...] if r == 0 else jnp.zeros((K1_DEV, LANES), jnp.float32)
        extra = jnp.where(lane == 0, exponent, jnp.where(lane == 1, counts - many * 1024, jnp.where(lane == 2, many, extra)))
        send_ref[pl.ds(r * K1_DEV, K1_DEV), pl.ds(depth, LANES)] = extra


def level1_kernel(*refs, dp, parts):
    pieces, (ids_ref, level1_ref, send_ref) = refs[:dp], refs[dp:]
    width = send_ref.shape[1]
    depth = width - LANES
    lane = lax.broadcasted_iota(jnp.int32, (K1_DEV, LANES), 1)
    for r in range(dp):
        terms, counts = [], []
        for q in range(dp):
            rows = pl.ds((r ^ q) * K1_DEV, K1_DEV)
            extra = pieces[q][rows, pl.ds(depth, LANES)]
            terms.append(pieces[q][rows, pl.ds(0, depth)] * (1.0 / power_of(extra[:, 0:1])))
            counts.append(extra[:, 1:2] + extra[:, 2:3] * 1024.0)
        while len(terms) > 1:
            terms = [a + b for a, b in zip(terms[::2], terms[1::2])]
            counts = [a + b for a, b in zip(counts[::2], counts[1::2])]
        level1 = terms[0] / jnp.maximum(counts[0], 1.0)
        if r == 0:
            level1_ref[...] = level1
        value, coarse, exponent = fitted(level1)
        rounded = value.astype(jnp.bfloat16).astype(jnp.float32)
        kept = coarse.astype(jnp.bfloat16).astype(jnp.float32) == rounded
        coded = jnp.where(kept, coarse, coarse + (rounded - coarse) * 0.25)
        send_ref[pl.ds(r * K1_DEV, K1_DEV), pl.ds(0, depth)] = coded
        mid = pieces[r][pl.ds(0, K1_DEV), pl.ds(depth, LANES)][:, 3:4]
        extra = jnp.where(lane == 0, exponent, jnp.where(lane == 1, mid, 0.0))
        for k in range(parts):
            extra = jnp.where(lane == 2 + k, ids_ref[:, 4 + k : 5 + k], extra)
        send_ref[pl.ds(r * K1_DEV, K1_DEV), pl.ds(depth, LANES)] = extra


def last_kernel(
    rows_ref, live_ref, *refs, origins, group, parts, pieces, tile
):
    gathered, (best_ref, level2_ref, level3_ref, high, low, half_norm, two, three, sems) = refs[:pieces], refs[pieces:]
    size, width = gathered[0].shape
    count = size * pieces
    depth = width - LANES
    second = group * K1_DEV * parts
    extra = jnp.concatenate([ref[:, pl.ds(depth, LANES)] for ref in gathered], axis=0)
    unscale = 1.0 / power_of(extra[:, 0:1])
    for i, ref in enumerate(gathered):
        rows = pl.ds(i * size, size)
        value = ref[:, pl.ds(0, depth)] * unscale[i * size : (i + 1) * size]
        upper = value.astype(jnp.bfloat16)
        wide = upper.astype(jnp.float32)
        high[rows, :] = upper
        low[rows, :] = (value - wide).astype(jnp.bfloat16)
        half_norm[rows, :] = 0.5 * jnp.sum(wide * wide, axis=1, keepdims=True)

    def total(chooser, upper, lower):
        dims = (((0,), (0,)), ((), ()))
        a = lax.dot_general(chooser, upper, dims, preferred_element_type=jnp.float32)
        b = lax.dot_general(chooser, lower, dims, preferred_element_type=jnp.float32)
        ones = jnp.ones((chooser.shape[0], LANES), jnp.bfloat16)
        n = lax.dot_general(chooser, ones, dims, preferred_element_type=jnp.float32)
        return (a + b) * jnp.concatenate([1.0 / n] * (depth // LANES), axis=1)

    mid = extra[:, 1:2].astype(jnp.int32)
    size = K1_DEV * parts
    owner = (mid // size) ^ lax.axis_index("group")
    inner = mid % size
    index = (inner // K1_DEV) * (group * K1_DEV) + owner * K1_DEV + inner % K1_DEV
    chooser = (index == lax.broadcasted_iota(jnp.int32, (count, second), 1)).astype(jnp.float32).astype(jnp.bfloat16)
    level2 = total(chooser, high[...], low[...])
    for k in range(parts):
        two[pl.ds(k * K1_DEV, K1_DEV), :] = level2[k * group * K1_DEV : k * group * K1_DEV + K1_DEV, :]
    order = [origins.index((0, q)) for q in range(group)]
    tops = [extra[p * K1_DEV : (p + 1) * K1_DEV, 2 + k : 3 + k] for k in range(parts) for p in order]
    top = jnp.concatenate(tops, axis=0).astype(jnp.int32)
    chooser = (top == lax.broadcasted_iota(jnp.int32, (second, K3), 1)).astype(jnp.float32).astype(jnp.bfloat16)
    upper = level2.astype(jnp.bfloat16)
    lower = (level2 - upper.astype(jnp.float32)).astype(jnp.bfloat16)
    three[...] = total(chooser, upper, lower)
    copies = [
        pltpu.make_async_copy(two, level2_ref, sems.at[0]),
        pltpu.make_async_copy(three, level3_ref, sems.at[1]),
    ]
    for c in copies:
        c.start()
    lane = lax.broadcasted_iota(jnp.int32, (1, LANES), 1)

    def scores(t, carry):
        score = lax.dot_general(
            high[...],
            live_ref[pl.ds(pl.multiple_of(t * tile, tile), tile), :],
            (((1,), (1,)), ((), ())),
            preferred_element_type=jnp.float32,
        )
        found = jnp.max(score - half_norm[...], axis=0, keepdims=True)
        for b in range(tile // LANES):
            g = t * (tile // LANES) + b
            best_ref[pl.ds(g, 1), :] = jnp.where(lane < rows_ref[g], found[:, b * LANES : (b + 1) * LANES], 0.0)
        return carry

    lax.fori_loop(0, live_ref.shape[0] // tile, scores, 0)
    for c in copies:
        c.wait()


def swap(values, mask, devices):
    return lax.ppermute(values, ALL, [(i, i ^ mask) for i in range(devices)])


def gather(values, group, devices):
    pieces, order, bit = [values], [0], group
    while bit > 1:
        step = min(4, bit)
        bit //= step
        masks = [bit * q for q in range(1, step)]
        pieces = pieces + [swap(p, m, devices) for m in masks for p in pieces]
        order = [q ^ m for m in [0] + masks for q in order]
    return pieces, order


def local(points, block_rows, block_owner, block_local, assign_mid, assign_top):
    dp, group = lax.axis_size("dp"), lax.axis_size("group")
    devices = dp * group
    rows, depth = points.shape
    blocks = block_rows.shape[0]
    parts = assign_top.shape[0] // K1_DEV
    width = depth + LANES
    smem = pl.BlockSpec(memory_space=pltpu.SMEM)
    vmem = pl.BlockSpec(memory_space=pltpu.VMEM)
    hbm = pl.BlockSpec(memory_space=pltpu.HBM)
    pieces = pl.pallas_call(
        functools.partial(sums_kernel, blocks=blocks, block_len=rows // blocks, dp=dp, group=group, parts=parts),
        out_shape=tuple(pltpu.VMEM((dp * SLOTS, width), jnp.float32) for _ in range(group))
        + (pltpu.VMEM((K1_DEV, LANES), jnp.float32), pltpu.VMEM((rows, depth), jnp.bfloat16)),
        in_specs=[hbm] * 6,
        out_specs=(vmem,) * (group + 2),
        scratch_shapes=[
            pltpu.VMEM((width // LANES, devices * SLOTS * 8, LANES), jnp.float32),
            pltpu.SMEM((blocks,), jnp.int32),
            pltpu.SMEM((blocks,), jnp.int32),
            pltpu.SMEM((blocks,), jnp.int32),
            pltpu.SMEM((K1_DEV,), jnp.int32),
            pltpu.SMEM((K1_DEV * parts,), jnp.int32),
            pltpu.SMEM((devices,), jnp.int32),
            pltpu.SemaphoreType.DMA((blocks,)),
            pltpu.SemaphoreType.DMA((5,)),
        ],
        compiler_params=pltpu.CompilerParams(vmem_limit_bytes=40 << 20),
        name="block_sums",
    )(block_rows, block_owner[:, 0], block_local, assign_mid[:, 0], assign_top[:, 0], points)
    ids, live = pieces[group:]
    got = [pieces[0]] + [swap(pieces[q], q, devices) for q in range(1, group)]
    own = pl.pallas_call(
        functools.partial(partial_kernel, dp=dp, group=group),
        out_shape=pltpu.VMEM((dp * K1_DEV, width), jnp.float32),
        in_specs=[vmem] * (group + 1),
        out_specs=vmem,
        compiler_params=pltpu.CompilerParams(vmem_limit_bytes=16 << 20),
        name="partial_sums",
    )(*got, ids)
    half = own.astype(jnp.float16)
    others = [swap(half, q * group, devices).astype(jnp.float32) for q in range(1, dp)]
    level1, send = pl.pallas_call(
        functools.partial(level1_kernel, dp=dp, parts=parts),
        out_shape=(
            jax.ShapeDtypeStruct((K1_DEV, depth), jnp.float32),
            pltpu.VMEM((dp * K1_DEV, width), jnp.float32),
        ),
        in_specs=[vmem] * (dp + 1),
        out_specs=(vmem, vmem),
        compiler_params=pltpu.CompilerParams(vmem_limit_bytes=16 << 20),
        name="level1",
    )(own, *others, ids)
    gathered, order = gather(send.astype(jnp.float16), group, devices)
    near = len(gathered) // 2
    gathered = [jnp.concatenate(gathered[:near], axis=0), jnp.concatenate(gathered[near:], axis=0)]
    origins = [(r, q) for q in order for r in range(dp)]
    best, level2, level3 = pl.pallas_call(
        functools.partial(
            last_kernel, origins=origins, group=group, parts=parts, pieces=len(gathered), tile=min(TILE, TILE * K3 // (devices * K1_DEV))
        ),
        out_shape=(
            jax.ShapeDtypeStruct((blocks, LANES), jnp.float32),
            jax.ShapeDtypeStruct((K1_DEV * parts, depth), jnp.float32),
            jax.ShapeDtypeStruct((K3, depth), jnp.float32),
        ),
        in_specs=[smem] + [vmem] * (1 + len(gathered)),
        out_specs=(vmem, pl.BlockSpec(memory_space=pl.ANY), pl.BlockSpec(memory_space=pl.ANY)),
        scratch_shapes=[
            pltpu.VMEM((devices * K1_DEV, depth), jnp.bfloat16),
            pltpu.VMEM((devices * K1_DEV, depth), jnp.bfloat16),
            pltpu.VMEM((devices * K1_DEV, 1), jnp.float32),
            pltpu.VMEM((K1_DEV * parts, depth), jnp.float32),
            pltpu.VMEM((K3, depth), jnp.float32),
            pltpu.SemaphoreType.DMA((2,)),
        ],
        compiler_params=pltpu.CompilerParams(vmem_limit_bytes=40 << 20),
        name="scores",
    )(block_rows, pltpu.with_memory_space_constraint(live, pltpu.VMEM), *[g.astype(jnp.float32) for g in gathered])
    return (level1, best.reshape(rows), level2, level3)


def solution(mesh):
    return jax.shard_map(
        local,
        mesh=mesh,
        in_specs=(
            P(("dp", "group"), None),
            P(("dp", "group")),
            P(("dp", "group"), None),
            P(("dp", "group")),
            P(("dp", "group"), None),
            P("group", None),
        ),
        out_specs=(P(("dp", "group"), None), P(("dp", "group")), P("group", None), P()),
        check_vma=False,
    )
```
